32 devices in a mesh: row: 8 (over z, y), col: 4 (over x, core).
Axes of the slice: x: 2, y: 2, z: 4, core: 2. Of those that a mesh axis runs over, the one named last changes fastest.
Arguments:
- rhs: float32 [65536, 256], P(('row', 'col')), may hold values from -6 to 6
- block_target: int32 [512], P(('row', 'col')), may hold values from 0 to 127, as said below
- pivot_inverse: float32 [32768, 1024], P(('row', 'col')), may hold values from -0.25 to 3, as said below
- update_factor: float32 [32768, 1024], P(('row', 'col')), may hold values from -0.1875 to 0.1875
- root_inverse: float32 [4096, 4096], P('row', 'col'), may hold values from -0.25 to 3, as said below
- update_map: int32 [256], P(('row', 'col')), may hold values from 0 to 31
Outputs:
- front_solution: float32 [32768, 256], P(('row', 'col'))
- root_solution: float32 [4096, 256], P(('row', 'col'))
The draws below stay inside these ranges and needn't reach their ends.
Inputs may be any that keep to these rules, and one draw needn't show every extreme that they name: block_target[g] is e * 16 + s: block g goes to the device of row index e in its own column, slot s there. Each device sends exactly 2 blocks to each of 8 devices of its column and none to the others; every slot of every device is filled exactly once. `pivot_inverse`: each device's block of 1024 rows is lower triangular with its diagonal positive. `root_inverse`: lower triangular with its diagonal positive.
All inputs are finite; a program needn't handle non-finite values.
Results may differ from the reference program's by a relative error of at most 0.000073.
Values sent between devices are 32-bit elements; how exact they have to be, the bound alone decides.
A program may use at most 192 MiB of HBM per device.

```python
import math
import jax
import jax.numpy as jnp
import numpy as np
from jax import lax

BLK = 128
NRHS = 256
RB_DEV = 16
CAP = 2
HALF = 1024
ROOT = 4096
N_ROW = 8
N_COL = 4
DEVICES = 32


def draw_block_target(key, part):
    base = jax.random.fold_in(key, 7)
    key_offset, key_local, key_slot = jax.random.split(base, 3)
    senders = RB_DEV // CAP
    offsets = jax.vmap(lambda single: jax.random.permutation(single, N_ROW)[:senders])(jax.random.split(key_offset, N_COL))
    ranks = jax.vmap(lambda single: jax.random.permutation(single, RB_DEV))(jax.random.split(key_local, DEVICES))
    shuffles = jax.vmap(lambda single: jax.random.permutation(single, RB_DEV))(jax.random.split(key_slot, DEVICES))
    device = jnp.arange(DEVICES, dtype=jnp.int32)
    row_index = device // N_COL
    col_index = device % N_COL
    group = ranks // CAP
    chosen = jnp.take_along_axis(offsets[col_index], group, axis=1)
    target_row = (row_index[:, None] + chosen) % N_ROW
    receiver = target_row * N_COL + col_index[:, None]
    slot_place = group * CAP + ranks % CAP
    slot_index = shuffles[receiver, slot_place]
    return (target_row * RB_DEV + slot_index).reshape(-1).astype(jnp.int32)


def lower_factor(key, leading, order):
    key_noise, key_diag = jax.random.split(jax.random.fold_in(key, 11))
    noise = jnp.clip(jax.random.normal(key_noise, (leading, order, order), jnp.float32) / math.sqrt(order), -0.25, 0.25)
    diagonal = jax.random.uniform(key_diag, (leading, order, 1), jnp.float32, 1.0, 2.0)
    rows_iota = jnp.arange(order)[:, None]
    cols_iota = jnp.arange(order)[None, :]
    return jnp.where(rows_iota == cols_iota, diagonal, jnp.where(rows_iota > cols_iota, noise, 0.0))


def draw_pivot_inverse(key, part):
    half = BLK * RB_DEV // 2
    return lower_factor(key, DEVICES, half).reshape(DEVICES * half, half)


def draw_root_inverse(key, part):
    return lower_factor(key, 1, ROOT).reshape(ROOT, ROOT)


def plant(array, rng, low, largest):
    shape = array.shape
    place = [jax.random.randint(jax.random.fold_in(rng, axis), (), 0, shape[axis]) for axis in range(len(shape))]
    array = array.at[tuple(place)].set(low)
    longest = shape.index(max(shape))
    place[longest] = (place[longest] + 1) % shape[longest]
    return array.at[tuple(place)].set(largest)


def block_scale(key, dims, shards, smallest, high):
    gain, own = 1.0, jax.random.fold_in(key, 6)
    for dim, blocks in shards:
        draws = jnp.exp(jax.random.uniform(jax.random.fold_in(own, dim), (blocks,), jnp.float32, smallest / len(shards), high / len(shards)))
        gain = gain * jnp.repeat(draws, dims[dim] // blocks).reshape([-1 if axis == dim else 1 for axis in range(len(dims))])
    return gain


def rank_table(amount, skew):
    weights = [(1 << 20) // math.isqrt(standing ** skew) + 1 for standing in range(1, amount + 1)]
    spread = 1 + sum(weights) // (1 << 30)
    return np.cumsum(np.array([max(1, weight // spread) for weight in weights]))


def ranked(own_key, extent, number_of, lean):
    table = rank_table(number_of, lean)
    lot = jax.random.randint(jax.random.fold_in(own_key, 1), extent, 0, int(table[number_of - 1]))
    standing = jnp.searchsorted(jnp.asarray(table, jnp.int32), lot, side="right")
    return jax.random.permutation(jax.random.fold_in(own_key, 2), number_of)[standing].astype(jnp.int32)


def centred(stream_key, dims, deviation, reach, pieces=(), kind=jnp.bfloat16):
    drawn = deviation * jax.random.normal(stream_key, dims, jnp.float32)
    if pieces:
        drawn = drawn * block_scale(stream_key, dims, pieces, -0.22, 0.18)
    return jnp.clip(drawn, -reach, reach).astype(kind)


def setup_inputs(seed: int = 0) -> dict:
    splits = jax.random.split(jax.random.key(seed), 7)
    rhs = centred(splits[0], (DEVICES * RB_DEV * BLK, NRHS), 1.0, 6.0, ((0, 32),), jnp.float32)
    block_target = draw_block_target(jax.random.fold_in(splits[6], 71), 0)
    pivot_inverse = draw_pivot_inverse(jax.random.fold_in(splits[6], 71), 0)
    update_factor = centred(splits[3], (DEVICES * HALF, HALF), HALF ** -0.5, 0.1875, ((0, 32),), jnp.float32)
    root_inverse = draw_root_inverse(jax.random.fold_in(splits[6], 71), 0)
    update_map = plant(ranked(splits[5], (DEVICES * RB_DEV // 2,), DEVICES, 2), jax.random.fold_in(splits[5], 3), 0, DEVICES - 1).astype(jnp.int32)
    return {"rhs": rhs, "block_target": block_target, "pivot_inverse": pivot_inverse, "update_factor": update_factor, "root_inverse": root_inverse, "update_map": update_map}


def reference(rhs, block_target, pivot_inverse, update_factor, root_inverse, update_map):
    count = DEVICES * RB_DEV
    block_index = jnp.arange(count, dtype=jnp.int32)
    column = (block_index // RB_DEV) % N_COL
    where_to = (((block_target // RB_DEV) * N_COL + column) * RB_DEV + block_target % RB_DEV).astype(jnp.int32)
    blocks = rhs.reshape(count, BLK, NRHS)
    fronts = jnp.zeros_like(blocks).at[where_to].set(blocks).reshape(DEVICES, RB_DEV * BLK, NRHS)
    half = BLK * RB_DEV // 2

    def front_step(operands):
        inverse, factor, front = operands
        solved = jnp.dot(inverse, front[:half], precision=lax.Precision.HIGHEST, preferred_element_type=jnp.float32)
        updated = front[half:] - jnp.dot(factor, solved, precision=lax.Precision.HIGHEST, preferred_element_type=jnp.float32)
        return solved, updated

    solved, updated = lax.map(front_step, (pivot_inverse.reshape(DEVICES, half, half), update_factor.reshape(DEVICES, half, half), fronts))
    root_rhs = jnp.zeros((DEVICES, BLK, NRHS), jnp.float32).at[update_map].add(updated.reshape(-1, BLK, NRHS)).reshape(ROOT, NRHS)
    root_solution = jnp.dot(root_inverse, root_rhs, precision=lax.Precision.HIGHEST, preferred_element_type=jnp.float32)
    return solved.reshape(DEVICES * half, NRHS), root_solution
```

```python
import functools
import jax
import jax.numpy as jnp
from jax import lax
from jax.experimental import pallas as pl
from jax.experimental.pallas import tpu as pltpu
from jax.sharding import PartitionSpec as P

BLK = 128
CAP = 2
CHUNKS = 16
MESH = pl.DeviceIdType.MESH
VMEM = pl.BlockSpec(memory_space=pltpu.VMEM)
SMEM = pl.BlockSpec(memory_space=pltpu.SMEM)


def split(value):
    high = value.astype(jnp.bfloat16)
    low = (value - high.astype(jnp.float32)).astype(jnp.bfloat16)
    return high, low


def dot3(a, b_high, b_low):
    a_high, a_low = split(a)
    total = jnp.dot(a_high, b_low, preferred_element_type=jnp.float32)
    total += jnp.dot(a_low, b_high, preferred_element_type=jnp.float32)
    return total + jnp.dot(a_high, b_high, preferred_element_type=jnp.float32)


def exchange_kernel(n_row, order, target_ref, rhs_ref, arrived, slots, staging, messages, send, recv, send_int, recv_int):
    me, col = lax.axis_index("row"), lax.axis_index("col")
    held = rhs_ref.shape[0]
    barrier = pltpu.get_barrier_semaphore()
    for k in order:
        pl.semaphore_signal(barrier, inc=1, device_id=(me ^ k, col), device_id_type=MESH)
    lane = lax.broadcasted_iota(jnp.int32, (8, 128), 1)
    targets = [target_ref[g] for g in range(held)]

    def chosen(peer):
        first, last = jnp.int32(held), jnp.int32(-1)
        slot_first, slot_last = jnp.int32(-1), jnp.int32(-1)
        for g in range(held):
            match = lax.div(targets[g], held) == peer
            fresh = jnp.logical_and(match, last < 0)
            first = jnp.where(fresh, g, first)
            slot_first = jnp.where(fresh, lax.rem(targets[g], held), slot_first)
            last = jnp.where(match, g, last)
            slot_last = jnp.where(match, lax.rem(targets[g], held), slot_last)
        return (
            jnp.minimum(first, held - 1),
            jnp.maximum(last, 0),
            jnp.where(lane == 0, slot_first, slot_last),
        )

    def stage(ref, place, peer):
        first, last, row = chosen(peer)
        ref[place, 0:BLK] = rhs_ref[first]
        ref[place, BLK : 2 * BLK] = rhs_ref[last]
        return row

    copies = []
    for place, k in enumerate(order):
        messages[place] = stage(staging, place, me ^ k)
        if place == 0:
            pl.semaphore_wait(barrier, n_row - 1)
        for source, target, ss, rs in (
            (staging, arrived, send, recv),
            (messages, slots, send_int, recv_int),
        ):
            copy = pltpu.make_async_remote_copy(
                src_ref=source.at[place],
                dst_ref=target.at[me],
                send_sem=ss.at[place],
                recv_sem=rs.at[place],
                device_id=(me ^ k, col),
                device_id_type=MESH,
            )
            copy.start()
            copies.append(copy)
    slots[me] = stage(arrived, me, me)
    for copy in copies:
        copy.wait()


def front_kernel(n_row, root_blocks, arrived, slots, update_map, pivot, factor, solved, dense, inverse, high, low):
    held = arrived.shape[0]
    rows = pivot.shape[0]
    tile = 2 * BLK
    half = rows // BLK
    for s in range(n_row):
        for rank in range(CAP):
            slot = slots[s, 0, rank]

            @pl.when(slot >= 0)
            def _():
                inverse[slot] = s * CAP + rank

    for b in range(half):
        part = pl.ds(b * BLK, BLK)
        high[part], low[part] = split(arrived[inverse[b]])

    @pl.loop(0, root_blocks)
    def _(b):
        dense[b] = jnp.zeros_like(dense[b])

    for start in range(0, rows, tile):
        deep = start + tile
        solved[start : start + tile] = dot3(pivot[start : start + tile, :deep], high[:deep], low[:deep])
    for start in range(0, rows, tile):
        part = pl.ds(start, tile)
        high[part], low[part] = split(solved[part])
    for start in range(0, rows, tile):
        product = dot3(factor[start : start + tile], high[...], low[...])
        for step in range(tile // BLK):
            b = start // BLK + step
            value = arrived[inverse[half + b]] - product[step * BLK : (step + 1) * BLK]
            dense[update_map[b]] += value


def root_kernel(
    n_row, n_col, skew, dense, inverse, out,
    got_core, got_x, y_up, y_down, y_us, y_ds, mid, z_up, z_down, z_us, z_ds,
    high, low, product, got_col,
    core_send, core_recv, x_send, x_recv, y_send, y_recv, z_send, z_recv, col_send, col_recv,
):
    n_y = max(1, n_col // 2)
    n_z, n_x = n_row // n_y, n_col // 2
    r, c = lax.axis_index("row"), lax.axis_index("col")
    z, y, x, k = r // n_y, r % n_y, c // 2, c % 2
    size = n_row * BLK
    step_rows = size // CHUNKS

    barrier = pltpu.get_barrier_semaphore()

    def greet(device):
        pl.semaphore_signal(barrier, inc=1, device_id=device, device_id_type=MESH)

    for d in range(1, n_col):
        greet((r, (c + d) % n_col))
    for pos, n, stride in ((y, n_y, 1), (z, n_z, n_y)):
        pl.when(pos > 0)(functools.partial(greet, (r - stride, c)))
        pl.when(pos < n - 1)(functools.partial(greet, (r + stride, c)))
    count = n_col - 1
    for pos, n in ((y, n_y), (z, n_z)):
        count = count + jnp.where(pos > 0, 1, 0) + jnp.where(pos < n - 1, 1, 0)
    pl.semaphore_wait(barrier, count)

    def remote(src, dst, ss, rs, device):
        return pltpu.make_async_remote_copy(
            src_ref=src, dst_ref=dst, send_sem=ss, recv_sem=rs, device_id=device, device_id_type=MESH
        )

    def rows_of(i):
        return pl.ds(pl.multiple_of(i * step_rows, step_rows), step_rows)

    def dense_rows(column, i):
        return pl.ds(pl.multiple_of(column * size + i * step_rows, step_rows), step_rows)

    partner = (r, c - k + (1 - k))
    base = got_core.at[0]

    def core_copy(d, i):
        xx = (x + d) % n_x
        return remote(
            dense.at[dense_rows(2 * xx + (1 - k), i)],
            got_core.at[d, rows_of(i)],
            core_send.at[d],
            core_recv.at[d, i],
            partner,
        )

    @pl.loop(0, CHUNKS)
    def _(i):
        for d in range(n_x - 1, -1, -1):
            core_copy(d, i).start()

    def x_copy(d, i):
        return remote(
            got_core.at[d, rows_of(i)],
            got_x.at[d - 1, rows_of(i)],
            x_send.at[d - 1],
            x_recv.at[d - 1, i],
            (r, ((x + d) % n_x) * 2 + k),
        )

    def stage_x(i):
        for d in range(n_x - 1, -1, -1):
            xx = (x + d) % n_x
            core_copy(d, i).wait_recv()
            value = dense[dense_rows(2 * xx + k, i)] + got_core[d, rows_of(i)]
            got_core[d, rows_of(i)] = value
            if d:
                x_copy(d, i).start()

    def join_x(i):
        value = base[rows_of(i)]
        for d in range(1, n_x):
            x_copy(d, i).wait_recv()
            value = value + got_x[d - 1, rows_of(i)]
        base[rows_of(i)] = value

    def line(n, pos, stride, held, up, down, us, ds, ss, rs):
        def send_up(i, source):
            return remote(source.at[rows_of(i)], up.at[rows_of(i)], ss.at[0], rs.at[0, i], (r + stride, c))

        def send_down(i, source):
            return remote(source.at[rows_of(i)], down.at[rows_of(i)], ss.at[1], rs.at[1, i], (r - stride, c))

        def hop(h, i):
            for place, landed, total, send in (
                (pos, up, us, send_up),
                (n - 1 - pos, down, ds, send_down),
            ):
                @pl.when(place == h)
                def _():
                    if h == 0:
                        send(i, held).start()
                    else:
                        send(i, total).wait_recv()
                        if h < n - 1:
                            total[rows_of(i)] = held[rows_of(i)] + landed[rows_of(i)]
                            send(i, total).start()

        def total(i, write):
            part = rows_of(i)

            @pl.when(pos == 0)
            def _():
                write(part, held[part] + down[part])

            @pl.when(pos == n - 1)
            def _():
                write(part, held[part] + up[part])

            if n > 2:
                @pl.when(jnp.logical_and(pos > 0, pos < n - 1))
                def _():
                    write(part, held[part] + up[part] + down[part])

        def drain():
            whole = pl.ds(0, size)

            @pl.when(pos < n - 1)
            def _():
                remote(held.at[whole], up.at[whole], ss.at[0], rs.at[0, 0], (r + stride, c)).wait_send()

            @pl.when(pos > 0)
            def _():
                remote(held.at[whole], down.at[whole], ss.at[1], rs.at[1, 0], (r - stride, c)).wait_send()

        return hop, total, drain

    y_hop, y_total, y_drain = line(n_y, y, 1, base, y_up, y_down, y_us, y_ds, y_send, y_recv)
    z_hop, z_total, z_drain = line(n_z, z, n_y, mid, z_up, z_down, z_us, z_ds, z_send, z_recv)

    def write_mid(part, value):
        mid[part] = value

    def write_split(part, value):
        high[part], low[part] = split(value)

    stages = [(0, stage_x)]
    at = skew

    def y_first(i):
        join_x(i)
        y_hop(0, i)

    stages.append((at, y_first))
    for h in range(1, n_y):
        at += skew
        if h < n_y - 1:
            stages.append((at, functools.partial(y_hop, h)))

    def z_first(i):
        y_hop(n_y - 1, i)
        y_total(i, write_mid)
        z_hop(0, i)

    stages.append((at, z_first))
    for h in range(1, n_z):
        at += skew
        if h < n_z - 1:
            stages.append((at, functools.partial(z_hop, h)))

    def z_last(i):
        z_hop(n_z - 1, i)
        z_total(i, write_split)

    stages.append((at, z_last))

    @pl.loop(0, CHUNKS + at)
    def _(t):
        for offset, stage in stages:
            i = t - offset

            @pl.when(jnp.logical_and(i >= 0, i < CHUNKS))
            def _():
                stage(i)

    tile = 2 * BLK
    for start in range(0, n_col * BLK, tile):
        product[start : start + tile] = dot3(inverse[start : start + tile], high[...], low[...])

    def col_copy(d):
        to = (c + d) % n_col
        return remote(
            product.at[pl.ds(pl.multiple_of(to * BLK, BLK), BLK)],
            got_col.at[d - 1],
            col_send.at[d - 1],
            col_recv.at[d - 1],
            (r, to),
        )

    for d in range(1, n_col):
        col_copy(d).start()
    value = product[pl.ds(pl.multiple_of(c * BLK, BLK), BLK)]
    for d in range(1, n_col):
        col_copy(d).wait_recv()
        value = value + got_col[d - 1]
    out[...] = value

    for d in range(1, n_col):
        col_copy(d).wait_send()
    for d in range(n_x):
        remote(
            dense.at[pl.ds(0, size)], got_core.at[d], core_send.at[d], core_recv.at[d, 0], partner
        ).wait_send()
    for d in range(1, n_x):
        remote(
            got_core.at[d], got_x.at[d - 1], x_send.at[d - 1], x_recv.at[d - 1, 0],
            (r, ((x + d) % n_x) * 2 + k),
        ).wait_send()
    y_drain()
    z_drain()


def shards(rhs, block_target, pivot_inverse, update_factor, root_inverse, update_map):
    n_row, n_col = lax.axis_size("row"), lax.axis_size("col")
    n_x = n_col // 2
    width = rhs.shape[1]
    held = rhs.shape[0] // BLK
    rows = pivot_inverse.shape[0]
    root_blocks = n_row * n_col
    size = n_row * BLK
    f32 = jnp.float32
    far = [k for k in range(n_row - 1, 0, -1)]
    half = n_row // 2
    near = [k for k in far if 1 < k < half]
    cross = [k for k in far if k >= half]
    order = []
    for place in range(max(len(near), len(cross))):
        order += near[place : place + 1] + cross[place : place + 1]
    order += [1]
    arrived, slots = pl.pallas_call(
        functools.partial(exchange_kernel, n_row, order),
        out_shape=(
            jax.ShapeDtypeStruct((n_row, CAP * BLK, width), f32),
            jax.ShapeDtypeStruct((n_row, 8, 128), jnp.int32),
        ),
        in_specs=[SMEM, VMEM],
        out_specs=(VMEM, VMEM),
        scratch_shapes=[
            pltpu.VMEM((n_row - 1, CAP * BLK, width), f32),
            pltpu.VMEM((n_row - 1, 8, 128), jnp.int32),
        ]
        + [pltpu.SemaphoreType.DMA((n_row - 1,))] * 4,
        compiler_params=pltpu.CompilerParams(collective_id=0, has_side_effects=True),
        name="exchange",
    )(block_target, rhs.reshape(held, BLK, width))
    solved, dense = pl.pallas_call(
        functools.partial(front_kernel, n_row, root_blocks),
        out_shape=(
            jax.ShapeDtypeStruct((rows, width), f32),
            jax.ShapeDtypeStruct((root_blocks, BLK, width), f32),
        ),
        in_specs=[VMEM, SMEM, SMEM, VMEM, VMEM],
        out_specs=(VMEM, VMEM),
        scratch_shapes=[
            pltpu.SMEM((held,), jnp.int32),
            pltpu.VMEM((rows, width), jnp.bfloat16),
            pltpu.VMEM((rows, width), jnp.bfloat16),
        ],
        name="front",
    )(arrived.reshape(n_row * CAP, BLK, width), slots, update_map, pivot_inverse, update_factor)
    slab = pltpu.VMEM((size, width), f32)
    root_solution = pl.pallas_call(
        functools.partial(root_kernel, n_row, n_col, 2),
        out_shape=jax.ShapeDtypeStruct((BLK, width), f32),
        in_specs=[VMEM, VMEM],
        out_specs=VMEM,
        scratch_shapes=[
            pltpu.VMEM((n_x, size, width), f32),
            pltpu.VMEM((n_x - 1, size, width), f32),
        ]
        + [slab] * 9
        + [
            pltpu.VMEM((size, width), jnp.bfloat16),
            pltpu.VMEM((size, width), jnp.bfloat16),
            pltpu.VMEM((n_col * BLK, width), f32),
            pltpu.VMEM((n_col - 1, BLK, width), f32),
            pltpu.SemaphoreType.DMA((n_x,)),
            pltpu.SemaphoreType.DMA((n_x, CHUNKS)),
            pltpu.SemaphoreType.DMA((n_x - 1,)),
            pltpu.SemaphoreType.DMA((n_x - 1, CHUNKS)),
            pltpu.SemaphoreType.DMA((2,)),
            pltpu.SemaphoreType.DMA((2, CHUNKS)),
            pltpu.SemaphoreType.DMA((2,)),
            pltpu.SemaphoreType.DMA((2, CHUNKS)),
            pltpu.SemaphoreType.DMA((n_col - 1,)),
            pltpu.SemaphoreType.DMA((n_col - 1,)),
        ],
        compiler_params=pltpu.CompilerParams(
            collective_id=1, has_side_effects=True, vmem_limit_bytes=67043328
        ),
        name="root",
    )(dense.reshape(root_blocks * BLK, width), root_inverse)
    return (solved, root_solution)


def solution(mesh):
    return jax.shard_map(
        shards,
        mesh=mesh,
        in_specs=(
            P(("row", "col"), None),
            P(("row", "col")),
            P(("row", "col"), None),
            P(("row", "col"), None),
            P("row", "col"),
            P(("row", "col")),
        ),
        out_specs=(P(("row", "col"), None), P(("row", "col"), None)),
        check_vma=False,
    )
```

```python
import functools
import jax
import jax.numpy as jnp
from jax import lax
from jax.experimental import pallas as pl
from jax.experimental.pallas import tpu as pltpu
from jax.sharding import PartitionSpec as P

BLK = 128
CAP = 2
CHUNKS = 32
CORE_SKEW = 2
LEAD = 6
SKEW = 4
MESH = pl.DeviceIdType.MESH
VMEM = pl.BlockSpec(memory_space=pltpu.VMEM)
SMEM = pl.BlockSpec(memory_space=pltpu.SMEM)
ANY = pl.BlockSpec(memory_space=pl.ANY)


def split(value):
    high = value.astype(jnp.bfloat16)
    low = (value - high.astype(jnp.float32)).astype(jnp.bfloat16)
    return high, low


def dot3(a, b_high, b_low):
    a_high, a_low = split(a)
    total = jnp.dot(a_high, b_low, preferred_element_type=jnp.float32)
    total += jnp.dot(a_low, b_high, preferred_element_type=jnp.float32)
    return total + jnp.dot(a_high, b_high, preferred_element_type=jnp.float32)


def forward_kernel(
    n_row, n_col, order, target_ref, map_ref, rhs_ref, pivot_hbm, factor_hbm, inverse_hbm,
    solved, out,
    staging, messages, arrived, slots, slots_smem, place_ref, weights, high, low, updated,
    give, got_core, got_x, y_up, y_down, y_ds, mid, z_up, z_down, z_ds, product, got_col,
    weight_sem, slot_sem, send, recv, send_int, recv_int,
    core_send, core_recv, x_send, x_recv, y_send, y_recv, z_send, z_recv, col_send, col_recv,
):
    n_y = max(1, n_col // 2)
    n_z, n_x = n_row // n_y, n_col // 2
    r, c = lax.axis_index("row"), lax.axis_index("col")
    z, y, x, k = r // n_y, r % n_y, c // 2, c % 2
    size = n_row * BLK
    step_rows = size // CHUNKS
    held = rhs_ref.shape[0]
    rows = solved.shape[0]
    half = rows // BLK
    tile = 2 * BLK
    base = got_core.at[0]

    def remote(src, dst, ss, rs, device):
        return pltpu.make_async_remote_copy(
            src_ref=src, dst_ref=dst, send_sem=ss, recv_sem=rs, device_id=device, device_id_type=MESH
        )

    barrier = pltpu.get_barrier_semaphore()
    for d in order:
        pl.semaphore_signal(barrier, inc=1, device_id=(r ^ d, c), device_id_type=MESH)
    for d in range(1, n_col):
        pl.semaphore_signal(barrier, inc=1, device_id=(r, (c + d) % n_col), device_id_type=MESH)

    pivot_copy = pltpu.make_async_copy(pivot_hbm, weights.at[pl.ds(0, rows)], weight_sem.at[0])
    factor_copy = pltpu.make_async_copy(factor_hbm, weights.at[pl.ds(rows, rows)], weight_sem.at[1])
    pivot_copy.start()
    factor_copy.start()

    lane = lax.broadcasted_iota(jnp.int32, (8, 128), 1)
    targets = [target_ref[g] for g in range(held)]

    def chosen(peer):
        first, last = jnp.int32(held), jnp.int32(-1)
        slot_first, slot_last = jnp.int32(-1), jnp.int32(-1)
        for g in range(held):
            match = lax.div(targets[g], held) == peer
            fresh = jnp.logical_and(match, last < 0)
            first = jnp.where(fresh, g, first)
            slot_first = jnp.where(fresh, lax.rem(targets[g], held), slot_first)
            last = jnp.where(match, g, last)
            slot_last = jnp.where(match, lax.rem(targets[g], held), slot_last)
        message = jnp.where(lane == 0, slot_first, slot_last)
        return jnp.minimum(first, held - 1), jnp.maximum(last, 0), message

    def data_copy(n, d):
        return remote(
            staging.at[n], arrived.at[pl.ds(r * CAP, CAP)], send.at[n], recv.at[n], (r ^ d, c)
        )

    def slot_copy(n, d):
        return remote(messages.at[n], slots.at[r], send_int.at[n], recv_int.at[n], (r ^ d, c))

    picks = []
    for n, d in enumerate(order):
        first, last, messages[n] = chosen(r ^ d)
        picks.append((first, last))
        staging[n, 0] = rhs_ref[first]
        staging[n, 1] = rhs_ref[last]
        if n == 0:
            pl.semaphore_wait(barrier, n_row + n_col - 2)
        slot_copy(n, d).start()
        data_copy(n, d).start()
    first, last, slots[r] = chosen(r)
    arrived[r * CAP] = rhs_ref[first]
    arrived[r * CAP + 1] = rhs_ref[last]

    for n, d in enumerate(order):
        slot_copy(n, d).wait_recv()
    to_smem = pltpu.make_async_copy(slots, slots_smem, slot_sem)
    to_smem.start()
    to_smem.wait()
    found = [slots_smem[s, 0, rank] for s in range(n_row) for rank in range(CAP)]
    for b in range(held):
        place = jnp.int32(0)
        for j, slot in enumerate(found):
            place = jnp.where(slot == b, j, place)
        place_ref[b] = place

    pivot_copy.wait()
    factor_copy.wait()
    for n, d in enumerate(order):
        data_copy(n, d).wait_recv()

    for b in range(half):
        part = pl.ds(b * BLK, BLK)
        high[part], low[part] = split(arrived[place_ref[b]])
    for start in range(0, rows, tile):
        deep = start + tile
        solved[start : start + tile] = dot3(weights[start : start + tile, :deep], high[:deep], low[:deep])
    for start in range(0, rows, tile):
        part = pl.ds(start, tile)
        high[part], low[part] = split(solved[part])
    for start in range(0, rows, tile):
        value = dot3(weights[rows + start : rows + start + tile], high[:rows], low[:rows])
        for step in range(tile // BLK):
            b = start // BLK + step
            updated[b] = arrived[place_ref[half + b]] - value[step * BLK : (step + 1) * BLK]

    deep = min(rows, size)
    inverse_copies = [
        pltpu.make_async_copy(
            inverse_hbm.at[:, pl.ds(n * deep, deep)],
            weights.at[pl.ds(n * n_col * BLK, n_col * BLK), pl.ds(0, deep)],
            weight_sem.at[n],
        )
        for n in range(size // deep)
    ]
    for copy in inverse_copies:
        copy.start()

    def rows_of(i):
        return pl.ds(pl.multiple_of(i * step_rows, step_rows), step_rows)

    per_block = BLK // step_rows
    maps = [map_ref[b] for b in range(half)]

    def dense(column, i):
        block = column * n_row + i // per_block
        part = pl.ds(pl.multiple_of((i % per_block) * step_rows, step_rows), step_rows)
        value = None
        for b in range(half):
            term = updated[b, part] * jnp.where(maps[b] == block, 1.0, 0.0)
            value = term if value is None else value + term
        return value

    partner = (r, c - k + (1 - k))

    def core_copy(d, i):
        return remote(
            give.at[d, rows_of(i)], got_core.at[d, rows_of(i)], core_send.at[d], core_recv.at[d, i], partner
        )

    def x_copy(d, i):
        return remote(
            got_core.at[d, rows_of(i)],
            got_x.at[d - 1, rows_of(i)],
            x_send.at[d - 1],
            x_recv.at[d - 1, i],
            (r, ((x + d) % n_x) * 2 + k),
        )

    def stage_core(i):
        for d in range(n_x - 1, -1, -1):
            give[d, rows_of(i)] = dense(2 * ((x + d) % n_x) + (1 - k), i)
            core_copy(d, i).start()

    def stage_x(i):
        for d in range(n_x - 1, -1, -1):
            value = dense(2 * ((x + d) % n_x) + k, i)
            core_copy(d, i).wait_recv()
            got_core[d, rows_of(i)] = value + got_core[d, rows_of(i)]
            if d:
                x_copy(d, i).start()

    def join_x(i):
        value = base[rows_of(i)]
        for d in range(1, n_x):
            x_copy(d, i).wait_recv()
            value = value + got_x[d - 1, rows_of(i)]
        base[rows_of(i)] = value

    def line(n, pos, stride, own, up, down, ds, ss, rs):
        def send_up(i, source):
            return remote(source.at[rows_of(i)], up.at[rows_of(i)], ss.at[0], rs.at[0, i], (r + stride, c))

        def send_down(i, source):
            return remote(source.at[rows_of(i)], down.at[rows_of(i)], ss.at[1], rs.at[1, i], (r - stride, c))

        def hop(h, i):
            for place, landed, total, go in (
                (pos, up, up, send_up),
                (n - 1 - pos, down, ds, send_down),
            ):
                @pl.when(place == h)
                def _():
                    if h == 0:
                        go(i, own).start()
                    else:
                        go(i, total).wait_recv()
                        if h < n - 1:
                            total[rows_of(i)] = own[rows_of(i)] + landed[rows_of(i)]
                            go(i, total).start()

        def total(i, write):
            part = rows_of(i)

            @pl.when(pos == 0)
            def _():
                write(part, own[part] + down[part])

            @pl.when(pos == n - 1)
            def _():
                write(part, own[part] + up[part])

            if n > 2:
                @pl.when(jnp.logical_and(pos > 0, pos < n - 1))
                def _():
                    write(part, up[part] + down[part])

        def drain():
            whole = pl.ds(0, size)

            @pl.when(pos < n - 1)
            def _():
                remote(own.at[whole], up.at[whole], ss.at[0], rs.at[0, 0], (r + stride, c)).wait_send()

            @pl.when(pos > 0)
            def _():
                remote(own.at[whole], down.at[whole], ss.at[1], rs.at[1, 0], (r - stride, c)).wait_send()

        return hop, total, drain

    y_hop, y_total, y_drain = line(n_y, y, 1, base, y_up, y_down, y_ds, y_send, y_recv)
    z_hop, z_total, z_drain = line(n_z, z, n_y, mid, z_up, z_down, z_ds, z_send, z_recv)

    def write_mid(part, value):
        mid[part] = value

    def write_split(part, value):
        high[part], low[part] = split(value)

    def y_first(i):
        join_x(i)
        y_hop(0, i)

    def z_first(i):
        y_hop(n_y - 1, i)
        y_total(i, write_mid)
        z_hop(0, i)

    def z_last(i):
        z_hop(n_z - 1, i)
        z_total(i, write_split)

    at = CORE_SKEW + LEAD
    stages = [(0, stage_core), (CORE_SKEW, stage_x), (at, y_first)]
    for h in range(1, n_y - 1):
        at += SKEW
        stages.append((at, functools.partial(y_hop, h)))
    at += SKEW
    stages.append((at, z_first))
    for h in range(1, n_z - 1):
        at += SKEW
        stages.append((at, functools.partial(z_hop, h)))
    at += SKEW
    stages.append((at, z_last))

    @pl.loop(0, CHUNKS + at)
    def _(t):
        for offset, stage in stages:
            i = t - offset

            @pl.when(jnp.logical_and(i >= 0, i < CHUNKS))
            def _():
                stage(i)

    for copy in inverse_copies:
        copy.wait()
    for start in range(0, n_col * BLK, tile):
        value = None
        for n in range(size // deep):
            part = slice(n * deep, (n + 1) * deep)
            at_row = n * n_col * BLK + start
            term = dot3(weights[at_row : at_row + tile, :deep], high[part], low[part])
            value = term if value is None else value + term
        product[start : start + tile] = value

    def col_copy(d):
        to = (c + d) % n_col
        return remote(
            product.at[pl.ds(pl.multiple_of(to * BLK, BLK), BLK)],
            got_col.at[d - 1],
            col_send.at[d - 1],
            col_recv.at[d - 1],
            (r, to),
        )

    for d in range(1, n_col):
        col_copy(d).start()
    value = product[pl.ds(pl.multiple_of(c * BLK, BLK), BLK)]
    for d in range(1, n_col):
        col_copy(d).wait_recv()
        value = value + got_col[d - 1]
    out[...] = value

    for n, d in enumerate(order):
        slot_copy(n, d).wait_send()
        data_copy(n, d).wait_send()
    for d in range(1, n_col):
        col_copy(d).wait_send()
    for d in range(n_x):
        remote(give.at[d], got_core.at[d], core_send.at[d], core_recv.at[d, 0], partner).wait_send()
    for d in range(1, n_x):
        remote(
            got_core.at[d], got_x.at[d - 1], x_send.at[d - 1], x_recv.at[d - 1, 0],
            (r, ((x + d) % n_x) * 2 + k),
        ).wait_send()
    y_drain()
    z_drain()


def shards(rhs, block_target, pivot_inverse, update_factor, root_inverse, update_map):
    n_row, n_col = lax.axis_size("row"), lax.axis_size("col")
    n_x = n_col // 2
    width = rhs.shape[1]
    held = rhs.shape[0] // BLK
    rows = pivot_inverse.shape[0]
    size = n_row * BLK
    f32 = jnp.float32
    half = n_row // 2
    near = list(range(half - 1, 1, -1))
    cross = list(range(n_row - 1, half - 1, -1))
    order = []
    for n in range(max(len(near), len(cross))):
        order += near[n : n + 1] + cross[n : n + 1]
    order += [1]
    slab = pltpu.VMEM((size, width), f32)
    longest = max(rows, size)
    dma = pltpu.SemaphoreType.DMA
    return pl.pallas_call(
        functools.partial(forward_kernel, n_row, n_col, order),
        out_shape=(
            jax.ShapeDtypeStruct((rows, width), f32),
            jax.ShapeDtypeStruct((BLK, width), f32),
        ),
        in_specs=[SMEM, SMEM, VMEM, ANY, ANY, ANY],
        out_specs=(VMEM, VMEM),
        scratch_shapes=[
            pltpu.VMEM((n_row - 1, CAP, BLK, width), f32),
            pltpu.VMEM((n_row - 1, 8, 128), jnp.int32),
            pltpu.VMEM((n_row * CAP, BLK, width), f32),
            pltpu.VMEM((n_row, 8, 128), jnp.int32),
            pltpu.SMEM((n_row, 8, 128), jnp.int32),
            pltpu.SMEM((held,), jnp.int32),
            pltpu.VMEM((2 * rows, rows), f32),
            pltpu.VMEM((longest, width), jnp.bfloat16),
            pltpu.VMEM((longest, width), jnp.bfloat16),
            pltpu.VMEM((rows // BLK, BLK, width), f32),
            pltpu.VMEM((n_x, size, width), f32),
            pltpu.VMEM((n_x, size, width), f32),
            pltpu.VMEM((n_x - 1, size, width), f32),
        ]
        + [slab] * 7
        + [
            pltpu.VMEM((n_col * BLK, width), f32),
            pltpu.VMEM((n_col - 1, BLK, width), f32),
            dma((2,)),
            dma(()),
        ]
        + [dma((n_row - 1,))] * 4
        + [
            dma((n_x,)),
            dma((n_x, CHUNKS)),
            dma((n_x - 1,)),
            dma((n_x - 1, CHUNKS)),
            dma((2,)),
            dma((2, CHUNKS)),
            dma((2,)),
            dma((2, CHUNKS)),
            dma((n_col - 1,)),
            dma((n_col - 1,)),
        ],
        compiler_params=pltpu.CompilerParams(
            collective_id=0, has_side_effects=True, vmem_limit_bytes=67043328
        ),
        name="forward",
    )(block_target, update_map, rhs.reshape(held, BLK, width), pivot_inverse, update_factor, root_inverse)


def solution(mesh):
    return jax.shard_map(
        shards,
        mesh=mesh,
        in_specs=(
            P(("row", "col"), None),
            P(("row", "col")),
            P(("row", "col"), None),
            P(("row", "col"), None),
            P("row", "col"),
            P(("row", "col")),
        ),
        out_specs=(P(("row", "col"), None), P(("row", "col"), None)),
        check_vma=False,
    )
```

```python
import functools
import jax
import jax.numpy as jnp
from jax import lax
from jax.experimental import pallas as pl
from jax.experimental.pallas import tpu as pltpu
from jax.sharding import PartitionSpec as P

BLK = 128
CAP = 2
PARTS = 2
CHUNKS = 16
CORE_SKEW = 2
LEAD = 6
SKEW = 4
MESH = pl.DeviceIdType.MESH
VMEM = pl.BlockSpec(memory_space=pltpu.VMEM)
SMEM = pl.BlockSpec(memory_space=pltpu.SMEM)
ANY = pl.BlockSpec(memory_space=pl.ANY)


def split(value):
    high = value.astype(jnp.bfloat16)
    low = (value - high.astype(jnp.float32)).astype(jnp.bfloat16)
    return high, low


def dot3(a, b_high, b_low):
    a_high, a_low = split(a)
    total = jnp.dot(a_high, b_low, preferred_element_type=jnp.float32)
    total += jnp.dot(a_low, b_high, preferred_element_type=jnp.float32)
    return total + jnp.dot(a_high, b_high, preferred_element_type=jnp.float32)


def forward_kernel(
    n_row, n_col, order, target_ref, map_ref, rhs_ref, pivot_hbm, factor_hbm, inverse_hbm,
    solved, out,
    staging, messages, arrived_a, arrived_b, slots, slots_smem, place_ref, weights, high, low, updated,
    give, got_core, got_x, y_up, y_down, y_ds, mid, z_up, z_down, z_ds, product, got_col,
    weight_sem, slot_sem, send, recv, send_int, recv_int,
    core_send, core_recv, x_send, x_recv, y_send, y_recv, z_send, z_recv, col_send, col_recv,
):
    n_y = max(1, n_col // 2)
    n_z, n_x = n_row // n_y, n_col // 2
    r, c = lax.axis_index("row"), lax.axis_index("col")
    z, y, x, k = r // n_y, r % n_y, c // 2, c % 2
    size = n_row * BLK
    step_rows = size // CHUNKS
    held = rhs_ref.shape[0]
    rows = solved.shape[0]
    half = rows // BLK
    tile = 2 * BLK
    base = got_core.at[0]
    arrived = (arrived_a, arrived_b)
    lanes = solved.shape[1] // PARTS

    def cols(h):
        return pl.ds(h * lanes, lanes)


    def remote(src, dst, ss, rs, device):
        return pltpu.make_async_remote_copy(
            src_ref=src, dst_ref=dst, send_sem=ss, recv_sem=rs, device_id=device, device_id_type=MESH
        )

    barrier = pltpu.get_barrier_semaphore()
    for d in order:
        pl.semaphore_signal(barrier, inc=1, device_id=(r ^ d, c), device_id_type=MESH)
    for d in range(1, n_col):
        pl.semaphore_signal(barrier, inc=1, device_id=(r, (c + d) % n_col), device_id_type=MESH)

    pivot_copy = pltpu.make_async_copy(pivot_hbm, weights.at[pl.ds(0, rows)], weight_sem.at[0])
    factor_copy = pltpu.make_async_copy(factor_hbm, weights.at[pl.ds(rows, rows)], weight_sem.at[1])
    pivot_copy.start()
    factor_copy.start()

    lane = lax.broadcasted_iota(jnp.int32, (8, 128), 1)
    targets = [target_ref[g] for g in range(held)]

    def chosen(peer):
        first, last = jnp.int32(held), jnp.int32(-1)
        slot_first, slot_last = jnp.int32(-1), jnp.int32(-1)
        for g in range(held):
            match = lax.div(targets[g], held) == peer
            fresh = jnp.logical_and(match, last < 0)
            first = jnp.where(fresh, g, first)
            slot_first = jnp.where(fresh, lax.rem(targets[g], held), slot_first)
            last = jnp.where(match, g, last)
            slot_last = jnp.where(match, lax.rem(targets[g], held), slot_last)
        message = jnp.where(lane == 0, slot_first, slot_last)
        return jnp.minimum(first, held - 1), jnp.maximum(last, 0), message

    def data_copy(n, d, h):
        return remote(
            staging.at[n, :, :, cols(h)],
            arrived[h].at[pl.ds(r * CAP, CAP)],
            send.at[h, n],
            recv.at[h, n],
            (r ^ d, c),
        )

    def slot_copy(n, d):
        return remote(messages.at[n], slots.at[r], send_int.at[n], recv_int.at[n], (r ^ d, c))

    picks = []
    for n, d in enumerate(order):
        first, last, messages[n] = chosen(r ^ d)
        picks.append((first, last))
        staging[n, 0] = rhs_ref[first]
        staging[n, 1] = rhs_ref[last]
        if n == 0:
            pl.semaphore_wait(barrier, n_row + n_col - 2)
        slot_copy(n, d).start()
        data_copy(n, d, 0).start()
    for h in range(1, PARTS):
        for n, d in enumerate(order):
            data_copy(n, d, h).start()
    first, last, slots[r] = chosen(r)
    for h in range(PARTS):
        arrived[h][r * CAP] = rhs_ref[first, :, cols(h)]
        arrived[h][r * CAP + 1] = rhs_ref[last, :, cols(h)]

    for n, d in enumerate(order):
        slot_copy(n, d).wait_recv()
    to_smem = pltpu.make_async_copy(slots, slots_smem, slot_sem)
    to_smem.start()
    to_smem.wait()
    found = [slots_smem[s, 0, rank] for s in range(n_row) for rank in range(CAP)]
    for b in range(held):
        place = jnp.int32(0)
        for j, slot in enumerate(found):
            place = jnp.where(slot == b, j, place)
        place_ref[b] = place

    pivot_copy.wait()
    factor_copy.wait()
    def front(h):
        for n, d in enumerate(order):
            data_copy(n, d, h).wait_recv()
        for b in range(half):
            part = pl.ds(b * BLK, BLK)
            high[part, cols(h)], low[part, cols(h)] = split(arrived[h][place_ref[b]])
        for start in range(0, rows, tile):
            deep = start + tile
            solved[start : start + tile, cols(h)] = dot3(
                weights[start : start + tile, :deep], high[:deep, cols(h)], low[:deep, cols(h)]
            )
        for start in range(0, rows, tile):
            part = pl.ds(start, tile)
            high[part, cols(h)], low[part, cols(h)] = split(solved[part, cols(h)])
        for start in range(0, rows, tile):
            value = dot3(
                weights[rows + start : rows + start + tile], high[:rows, cols(h)], low[:rows, cols(h)]
            )
            for step in range(tile // BLK):
                b = start // BLK + step
                updated[b, :, cols(h)] = (
                    arrived[h][place_ref[half + b]] - value[step * BLK : (step + 1) * BLK]
                )

    deep = min(rows, size)
    inverse_copies = [
        pltpu.make_async_copy(
            inverse_hbm.at[:, pl.ds(n * deep, deep)],
            weights.at[pl.ds(n * n_col * BLK, n_col * BLK), pl.ds(0, deep)],
            weight_sem.at[n],
        )
        for n in range(size // deep)
    ]
    def rows_of(i):
        return pl.ds(pl.multiple_of(i * step_rows, step_rows), step_rows)

    per_block = BLK // step_rows
    maps = [map_ref[b] for b in range(half)]

    partner = (r, c - k + (1 - k))

    def root(h):
        def dense(column, i):
            block = column * n_row + i // per_block
            part = pl.ds(pl.multiple_of((i % per_block) * step_rows, step_rows), step_rows)
            value = None
            for b in range(half):
                term = updated[b, part, cols(h)] * jnp.where(maps[b] == block, 1.0, 0.0)
                value = term if value is None else value + term
            return value

        def core_copy(d, i):
            return remote(
                give.at[d, rows_of(i), cols(h)], got_core.at[d, rows_of(i), cols(h)], core_send.at[h, d], core_recv.at[h, d, i], partner
            )

        def x_copy(d, i):
            return remote(
                got_core.at[d, rows_of(i), cols(h)],
                got_x.at[d - 1, rows_of(i), cols(h)],
                x_send.at[h, d - 1],
                x_recv.at[h, d - 1, i],
                (r, ((x + d) % n_x) * 2 + k),
            )

        def stage_core(i):
            for d in range(n_x - 1, -1, -1):
                give[d, rows_of(i), cols(h)] = dense(2 * ((x + d) % n_x) + (1 - k), i)
                core_copy(d, i).start()

        def stage_x(i):
            for d in range(n_x - 1, -1, -1):
                value = dense(2 * ((x + d) % n_x) + k, i)
                core_copy(d, i).wait_recv()
                got_core[d, rows_of(i), cols(h)] = value + got_core[d, rows_of(i), cols(h)]
                if d:
                    x_copy(d, i).start()

        def join_x(i):
            value = base[rows_of(i), cols(h)]
            for d in range(1, n_x):
                x_copy(d, i).wait_recv()
                value = value + got_x[d - 1, rows_of(i), cols(h)]
            base[rows_of(i), cols(h)] = value

        def line(n, pos, stride, own, up, down, ds, ss, rs):
            def send_up(i, source):
                return remote(source.at[rows_of(i), cols(h)], up.at[rows_of(i), cols(h)], ss.at[h, 0], rs.at[h, 0, i], (r + stride, c))

            def send_down(i, source):
                return remote(source.at[rows_of(i), cols(h)], down.at[rows_of(i), cols(h)], ss.at[h, 1], rs.at[h, 1, i], (r - stride, c))

            def hop(step, i):
                for place, landed, total, go in (
                    (pos, up, up, send_up),
                    (n - 1 - pos, down, ds, send_down),
                ):
                    @pl.when(place == step)
                    def _():
                        if step == 0:
                            go(i, own).start()
                        else:
                            go(i, total).wait_recv()
                            if step < n - 1:
                                total[rows_of(i), cols(h)] = own[rows_of(i), cols(h)] + landed[rows_of(i), cols(h)]
                                go(i, total).start()

            def total(i, write):
                part = rows_of(i)

                @pl.when(pos == 0)
                def _():
                    write(part, own[part, cols(h)] + down[part, cols(h)])

                @pl.when(pos == n - 1)
                def _():
                    write(part, own[part, cols(h)] + up[part, cols(h)])

                if n > 2:
                    @pl.when(jnp.logical_and(pos > 0, pos < n - 1))
                    def _():
                        write(part, up[part, cols(h)] + down[part, cols(h)])

            def drain():
                whole = pl.ds(0, size)

                @pl.when(pos < n - 1)
                def _():
                    remote(own.at[whole, cols(h)], up.at[whole, cols(h)], ss.at[h, 0], rs.at[h, 0, 0], (r + stride, c)).wait_send()

                @pl.when(pos > 0)
                def _():
                    remote(own.at[whole, cols(h)], down.at[whole, cols(h)], ss.at[h, 1], rs.at[h, 1, 0], (r - stride, c)).wait_send()

            return hop, total, drain

        y_hop, y_total, y_drain = line(n_y, y, 1, base, y_up, y_down, y_ds, y_send, y_recv)
        z_hop, z_total, z_drain = line(n_z, z, n_y, mid, z_up, z_down, z_ds, z_send, z_recv)

        def write_mid(part, value):
            mid[part, cols(h)] = value

        def write_split(part, value):
            high[part, cols(h)], low[part, cols(h)] = split(value)

        def y_first(i):
            join_x(i)
            y_hop(0, i)

        def z_first(i):
            y_hop(n_y - 1, i)
            y_total(i, write_mid)
            z_hop(0, i)

        def z_last(i):
            z_hop(n_z - 1, i)
            z_total(i, write_split)

        def drain():
            for d in range(n_x):
                remote(
                    give.at[d, :, cols(h)], got_core.at[d, :, cols(h)],
                    core_send.at[h, d], core_recv.at[h, d, 0], partner,
                ).wait_send()
            for d in range(1, n_x):
                remote(
                    got_core.at[d, :, cols(h)], got_x.at[d - 1, :, cols(h)],
                    x_send.at[h, d - 1], x_recv.at[h, d - 1, 0],
                    (r, ((x + d) % n_x) * 2 + k),
                ).wait_send()
            y_drain()
            z_drain()

        at = CORE_SKEW + LEAD
        head = [(0, stage_core), (CORE_SKEW, stage_x), (at, y_first)]
        for step in range(1, n_y - 1):
            at += SKEW
            head.append((at, functools.partial(y_hop, step)))
        head.append((at + SKEW, z_first))
        tail = [((step - 1) * SKEW, functools.partial(z_hop, step)) for step in range(1, n_z - 1)]
        tail.append(((n_z - 2) * SKEW, z_last))
        return head, tail, drain

    def run(stages):
        @pl.loop(0, CHUNKS + max(offset for offset, _ in stages))
        def _(t):
            for offset, stage in stages:
                i = t - offset

                @pl.when(jnp.logical_and(i >= 0, i < CHUNKS))
                def _():
                    stage(i)

    parts = [root(h) for h in range(PARTS)]
    left = []
    for h, (head, tail, _) in enumerate(parts):
        front(h)
        if h == PARTS - 1:
            for copy in inverse_copies:
                copy.start()
            after = max(offset for offset, _ in head) + SKEW
            tail = [(after + offset, stage) for offset, stage in tail]
            run(left + head + tail)
        else:
            run(left + head)
            left = tail

    for copy in inverse_copies:
        copy.wait()
    for start in range(0, n_col * BLK, tile):
        value = None
        for n in range(size // deep):
            part = slice(n * deep, (n + 1) * deep)
            at_row = n * n_col * BLK + start
            term = dot3(weights[at_row : at_row + tile, :deep], high[part], low[part])
            value = term if value is None else value + term
        product[start : start + tile] = value

    def col_copy(d):
        to = (c + d) % n_col
        return remote(
            product.at[pl.ds(pl.multiple_of(to * BLK, BLK), BLK)],
            got_col.at[d - 1],
            col_send.at[d - 1],
            col_recv.at[d - 1],
            (r, to),
        )

    for d in range(1, n_col):
        col_copy(d).start()
    value = product[pl.ds(pl.multiple_of(c * BLK, BLK), BLK)]
    for d in range(1, n_col):
        col_copy(d).wait_recv()
        value = value + got_col[d - 1]
    out[...] = value

    for n, d in enumerate(order):
        slot_copy(n, d).wait_send()
        for h in range(PARTS):
            data_copy(n, d, h).wait_send()
    for d in range(1, n_col):
        col_copy(d).wait_send()
    for _, _, drain in parts:
        drain()


def shards(rhs, block_target, pivot_inverse, update_factor, root_inverse, update_map):
    n_row, n_col = lax.axis_size("row"), lax.axis_size("col")
    n_x = n_col // 2
    width = rhs.shape[1]
    held = rhs.shape[0] // BLK
    rows = pivot_inverse.shape[0]
    size = n_row * BLK
    f32 = jnp.float32
    half = n_row // 2
    near = list(range(half - 1, 1, -1))
    cross = list(range(n_row - 1, half - 1, -1))
    order = []
    for n in range(max(len(near), len(cross))):
        order += near[n : n + 1] + cross[n : n + 1]
    order += [1]
    slab = pltpu.VMEM((size, width), f32)
    longest = max(rows, size)
    dma = pltpu.SemaphoreType.DMA
    return pl.pallas_call(
        functools.partial(forward_kernel, n_row, n_col, order),
        out_shape=(
            jax.ShapeDtypeStruct((rows, width), f32),
            jax.ShapeDtypeStruct((BLK, width), f32),
        ),
        in_specs=[SMEM, SMEM, VMEM, ANY, ANY, ANY],
        out_specs=(VMEM, VMEM),
        scratch_shapes=[
            pltpu.VMEM((n_row - 1, CAP, BLK, width), f32),
            pltpu.VMEM((n_row - 1, 8, 128), jnp.int32),
            pltpu.VMEM((n_row * CAP, BLK, width // PARTS), f32),
            pltpu.VMEM((n_row * CAP, BLK, width // PARTS), f32),
            pltpu.VMEM((n_row, 8, 128), jnp.int32),
            pltpu.SMEM((n_row, 8, 128), jnp.int32),
            pltpu.SMEM((held,), jnp.int32),
            pltpu.VMEM((2 * rows, rows), f32),
            pltpu.VMEM((longest, width), jnp.bfloat16),
            pltpu.VMEM((longest, width), jnp.bfloat16),
            pltpu.VMEM((rows // BLK, BLK, width), f32),
            pltpu.VMEM((n_x, size, width), f32),
            pltpu.VMEM((n_x, size, width), f32),
            pltpu.VMEM((n_x - 1, size, width), f32),
        ]
        + [slab] * 7
        + [
            pltpu.VMEM((n_col * BLK, width), f32),
            pltpu.VMEM((n_col - 1, BLK, width), f32),
            dma((2,)),
            dma(()),
        ]
        + [dma((PARTS, n_row - 1))] * 2
        + [dma((n_row - 1,))] * 2
        + [
            dma((PARTS, n_x)),
            dma((PARTS, n_x, CHUNKS)),
            dma((PARTS, n_x - 1)),
            dma((PARTS, n_x - 1, CHUNKS)),
            dma((PARTS, 2)),
            dma((PARTS, 2, CHUNKS)),
            dma((PARTS, 2)),
            dma((PARTS, 2, CHUNKS)),
            dma((n_col - 1,)),
            dma((n_col - 1,)),
        ],
        compiler_params=pltpu.CompilerParams(
            collective_id=0, has_side_effects=True, vmem_limit_bytes=67043328
        ),
        name="forward",
    )(block_target, update_map, rhs.reshape(held, BLK, width), pivot_inverse, update_factor, root_inverse)


def solution(mesh):
    return jax.shard_map(
        shards,
        mesh=mesh,
        in_specs=(
            P(("row", "col"), None),
            P(("row", "col")),
            P(("row", "col"), None),
            P(("row", "col"), None),
            P("row", "col"),
            P(("row", "col")),
        ),
        out_specs=(P(("row", "col"), None), P(("row", "col"), None)),
        check_vma=False,
    )
```
